512 devices in a mesh: row: 16 (over z_lo, y), col: 32 (over x, z_hi, core).
Axes of the slice: x: 4, y: 8, z: 8 (z_hi: 4, z_lo: 2; z = z_hi * 2 + z_lo), core: 2. Of those that a mesh axis runs over, the one named last changes fastest.
Arguments:
- amplitudes: bfloat16 [4096, 262144], P(None, ('row', 'col')), may hold values from -6 to 6
- integrals: bfloat16 [256, 262144], P(None, ('row', 'col')), may hold values from -6 to 6
- hh_coupling: bfloat16 [256, 4096], P('row'), may hold values from -0.09375 to 0.09375
- thc_factor: bfloat16 [512, 1024], P(None, ('row', 'col')), may hold values from -0.25 to 0.25
- thc_core: float32 [1024, 1024], P('col', 'row'), may hold values from -3 to 3
- occ_energy: float32 [64], replicated, may hold values from -2 to -0.5
- vir_energy: float32 [512], replicated, may hold values from 0.3 to 3
- pair_owner: int32 [256], replicated, may hold values from 0 to 4095, as said below
Outputs:
- updated: bfloat16 [256, 262144], P(None, ('row', 'col'))
The draws below stay inside these ranges and needn't reach their ends.
Inputs may be any that keep to these rules, and one draw needn't show every extreme that they name: pair_owner holds 256 distinct occupied pairs.
All inputs are finite; a program needn't handle non-finite values.
Results may differ from the reference program's by a relative error of at most 0.007.
Values may be sent and summed in bfloat16 or wider, within the bound.
A program may use at most 64 MiB of HBM per device.

```python
import math
import jax
import jax.numpy as jnp
from jax import lax

OCC = 64
VIR = 512
NPTS = 1024
PC = 8
PW = 256
N_ROW = 16
N_COL = 32


def draw_pair_owner(key, part):
    return jax.random.permutation(key, OCC * OCC)[:PW].astype(jnp.int32)


def steps_of(key, dims, cuts, low, high):
    factor_of = 1.0
    for axis_at, shards_of in cuts:
        heights = jax.random.uniform(jax.random.fold_in(jax.random.fold_in(key, 6), axis_at), (shards_of,), jnp.float32, low / len(cuts), high / len(cuts))
        factor_of = factor_of * jnp.repeat(jnp.exp(heights), dims[axis_at] // shards_of).reshape((-1,) + (1,) * (len(dims) - 1 - axis_at))
    return factor_of


def bell_draw(stream_key, dims, deviation, most, split=(), dtype=jnp.bfloat16):
    array = deviation * jax.random.normal(stream_key, dims, jnp.float32)
    if split:
        array = array * steps_of(stream_key, dims, split, -0.22, 0.18)
    return jnp.clip(array, -most, most).astype(dtype)


def setup_inputs(seed: int = 0) -> dict:
    key_list = jax.random.split(jax.random.key(seed), 9)
    return {
        "amplitudes": bell_draw(key_list[0], (OCC * OCC, VIR * VIR), 1.0, 6.0, ((1, 512),)),
        "integrals": bell_draw(key_list[1], (PW, VIR * VIR), 1.0, 6.0, ((1, 512),)),
        "hh_coupling": bell_draw(key_list[2], (PW, OCC * OCC), (OCC * OCC) ** -0.5, 0.09375, ((0, 16),)),
        "thc_factor": bell_draw(key_list[3], (VIR, NPTS), VIR ** -0.5, 0.25, ((1, 512),)),
        "thc_core": bell_draw(key_list[4], (NPTS, NPTS), 0.5, 3.0, ((0, 32), (1, 16)), jnp.float32),
        "occ_energy": jnp.clip(jax.random.uniform(key_list[5], (OCC,), jnp.float32, -2.0, -0.5), -2.0, -0.5),
        "vir_energy": jnp.clip(jnp.exp(jax.random.uniform(key_list[6], (VIR,), jnp.float32, math.log(0.3), math.log(3.0))), 0.3, 3.0),
        "pair_owner": draw_pair_owner(jax.random.fold_in(key_list[8], 71), 0),
    }


def ladder_block(amps_block, thc_factor, thc_core):
    factor = thc_factor.astype(jnp.float32)
    block_points = NPTS // N_ROW
    half = jnp.einsum('pcd,dq->pcq', amps_block.astype(jnp.float32), factor).astype(jnp.bfloat16)
    middle = jnp.einsum('cP,pcq->pPq', factor, half.astype(jnp.float32))
    weighted = (thc_core[None] * middle).astype(jnp.bfloat16)
    back = jnp.einsum('aP,pPq->paq', factor, weighted.astype(jnp.float32)).astype(jnp.bfloat16)
    back_split = back.astype(jnp.float32).reshape(PC, VIR, N_ROW, block_points)
    factor_split = factor.reshape(VIR, N_ROW, block_points)
    partial_value = jnp.einsum('parq,brq->rpab', back_split, factor_split).astype(jnp.bfloat16)
    partial_value = lax.optimization_barrier(partial_value)
    return jnp.sum(partial_value.astype(jnp.float32), axis=0).astype(jnp.bfloat16)


def reference(amplitudes, integrals, hh_coupling, thc_factor, thc_core, occ_energy, vir_energy, pair_owner):
    coupled = jnp.dot(hh_coupling, amplitudes, preferred_element_type=jnp.float32)
    owned = amplitudes[pair_owner]
    blocks = owned.reshape(N_COL, PC, VIR, VIR)
    ladder = lax.map(lambda blk: ladder_block(blk, thc_factor, thc_core), blocks)
    ladder = ladder.reshape(PW, VIR * VIR)
    first_occ = occ_energy[pair_owner // OCC]
    second_occ = occ_energy[pair_owner % OCC]
    vir_pairs = (vir_energy[:, None] + vir_energy[None, :]).reshape(1, VIR * VIR)
    denom = vir_pairs - (first_occ + second_occ)[:, None]
    rest = (integrals.astype(jnp.float32) + coupled) + ladder.astype(jnp.float32)
    update = 0.4 * owned.astype(jnp.float32) + 0.6 * rest / denom
    return update.astype(jnp.bfloat16)
```

```python
import jax
import jax.numpy as jnp
from jax import lax
from jax.experimental import pallas as pl
from jax.experimental.pallas import tpu as pltpu
from jax.sharding import Mesh
from jax.sharding import PartitionSpec as P

AXES = ("zl", "y", "x", "zh", "core")
ROW = ("zl", "y")
COL = ("x", "zh", "core")
BF = jnp.bfloat16
F32 = jnp.float32
N_EXCHANGES = 24


def nt(a, b):
    return lax.dot_general(a, b, (((1,), (1,)), ((), ())), preferred_element_type=F32)


def nn(a, b):
    return jnp.dot(a, b, preferred_element_type=F32)


def iota(shape, dim):
    return lax.broadcasted_iota(jnp.int32, shape, dim)


def swap_matrix():
    i, j = iota((256, 256), 0), iota((256, 256), 1)
    return (j == (i % 16) * 16 + i // 16).astype(F32).astype(BF)


def order_matrix():
    p, c = iota((512, 512), 0), iota((512, 512), 1)
    return (c == (p % 16) * 32 + ((p // 16) % 16) * 2 + p // 256).astype(F32).astype(BF)


class Exchange:
    def __init__(self, sems, number, count, me, where, src, dst):
        self.send, self.recv = sems
        self.number, self.count, self.me = number, count, me
        self.where, self.src, self.dst = where, src, dst

    def copy(self, d, to, slot):
        return pltpu.make_async_remote_copy(
            src_ref=self.src(to),
            dst_ref=self.dst(slot),
            send_sem=self.send.at[self.number, d],
            recv_sem=self.recv.at[self.number, d],
            device_id=self.where(to),
            device_id_type=pl.DeviceIdType.MESH,
        )

    def each(self, act):
        def step(d, carry):
            act(d)
            return carry

        lax.fori_loop(1, self.count, step, 0)

    def start(self):
        def act(d):
            self.copy(d, lax.rem(self.me + d, self.count), self.me).start()

        self.each(act)

    def wait_recv(self):
        def act(d):
            source = lax.rem(self.me + self.count - d, self.count)
            self.copy(d, source, source).wait_recv()

        self.each(act)

    def wait_send(self):
        def act(d):
            self.copy(d, lax.rem(self.me + d, self.count), self.me).wait_send()

        self.each(act)


class RingOfFour:
    def __init__(self, sems, number, me, block, half):
        self.send, self.recv = sems
        self.number, self.me = number, me
        self.block, self.half = block, half

    def copy(self, part, ref, to):
        return pltpu.make_async_remote_copy(
            src_ref=ref,
            dst_ref=ref,
            send_sem=self.send.at[self.number, part],
            recv_sem=self.recv.at[self.number, part],
            device_id={"x": to},
            device_id_type=pl.DeviceIdType.MESH,
        )

    def members(self):
        return lax.rem(self.me + 1, 4), lax.rem(self.me + 2, 4), lax.rem(self.me + 3, 4)

    def start(self):
        right, _, left = self.members()
        self.copy(0, self.block(self.me), right).start()
        self.copy(1, self.block(self.me), left).start()

    def forward(self):
        right, _, left = self.members()
        self.copy(0, self.block(left), right).wait_recv()
        self.copy(2, self.half(left, 0), right).start()
        self.copy(1, self.block(right), left).wait_recv()
        self.copy(3, self.half(right, 1), left).start()

    def wait_recv(self):
        right, across, left = self.members()
        self.copy(2, self.half(across, 0), right).wait_recv()
        self.copy(3, self.half(across, 1), left).wait_recv()

    def wait_send(self):
        right, _, left = self.members()
        self.copy(0, self.block(self.me), right).wait_send()
        self.copy(1, self.block(self.me), left).wait_send()
        self.copy(2, self.half(left, 0), right).wait_send()
        self.copy(3, self.half(right, 1), left).wait_send()


class Swap:
    def __init__(self, sems, number, core, src, dst):
        self.send, self.recv = sems
        self.number, self.core = number, core
        self.src, self.dst = src, dst

    def copy(self, slot):
        return pltpu.make_async_remote_copy(
            src_ref=self.src,
            dst_ref=self.dst(slot),
            send_sem=self.send.at[self.number, 0],
            recv_sem=self.recv.at[self.number, 0],
            device_id={"core": 1 - self.core},
            device_id_type=pl.DeviceIdType.MESH,
        )

    def start(self):
        self.copy(self.core).start()

    def wait_recv(self):
        self.copy(1 - self.core).wait_recv()

    def wait_send(self):
        self.copy(self.core).wait_send()


def kernel(
    amp_hbm, integrals, hh, factor, core_in, occ, vir, owner, out,
    amp, own, own0, own1, in0, in1, mid0, mid1, fin0, fin1, whole,
    chunk, pieces, points, core_parts, core_block, rows, half, order0, order1,
    ladder, give, take, lad0, lad1, got0, got1, turn0, turn1, back0, back1,
    coupled, amp_sem, send_sems, recv_sems,
):
    zl, y, x, zh, core = (lax.axis_index(a) for a in AXES)
    r, xz = zl * 8 + y, x * 4 + zh
    other = 1 - core
    sems = (send_sems, recv_sems)
    MESH = pl.DeviceIdType.MESH

    def row_at(t):
        return {"zl": t // 8, "y": t % 8}

    def col_at(t):
        return {"x": t // 4, "zh": t % 4}

    def zh_at(t):
        return {"zh": t}

    fetch = pltpu.make_async_copy(amp_hbm, amp, amp_sem)
    fetch.start()

    barrier = pltpu.get_barrier_semaphore()

    def greet_row(d, carry):
        pl.semaphore_signal(
            barrier, inc=1, device_id=row_at(lax.rem(r + d, 16)), device_id_type=MESH
        )
        return carry

    def greet_col(d, carry):
        pl.semaphore_signal(
            barrier, inc=1, device_id=col_at(lax.rem(xz + d, 16)), device_id_type=MESH
        )
        return carry

    lax.fori_loop(1, 16, greet_row, 0)
    lax.fori_loop(1, 16, greet_col, 0)
    for d in range(4):
        pl.semaphore_signal(
            barrier,
            inc=1,
            device_id={"zh": lax.rem(zh + d, 4), "core": other},
            device_id_type=MESH,
        )

    for k in range(2):
        chunk[k] = factor[:, k * 256 : k * 256 + 256].astype(F32)
    core_parts[x, zh, r] = jnp.concatenate(
        [core_in[0:16, :], core_in[16:32, :]], axis=1
    ).astype(BF)
    tile = pl.ds(pl.multiple_of((core * 16 + xz) * 128, 128), 128)
    lanes = pl.ds(pl.multiple_of(zh * 128, 128), 128)
    rows[core, x, r, :, lanes] = hh[:, tile]
    swap = swap_matrix()

    pl.semaphore_wait(barrier, 34)

    def piece(d, c, to_zh, to_core, slot_zh, slot_core):
        return pltpu.make_async_remote_copy(
            src_ref=chunk.at[to_core],
            dst_ref=pieces.at[slot_zh, slot_core],
            send_sem=send_sems.at[0, d * 2 + c],
            recv_sem=recv_sems.at[0, d * 2 + c],
            device_id={"zh": to_zh, "core": to_core},
            device_id_type=MESH,
        )

    hops = [(d, c) for d in range(4) for c in range(2) if d or c]

    def piece_out(d, c):
        return piece(d, c, lax.rem(zh + d, 4), core if c == 0 else other, zh, core)

    def piece_in(d, c):
        from_zh, from_core = lax.rem(zh + 4 - d, 4), core if c == 0 else other
        return piece(d, c, from_zh, from_core, from_zh, from_core)

    for d, c in hops:
        piece_out(d, c).start()
    pieces[zh, core] = chunk[core]

    core_zh = Exchange(
        sems, 1, 4, zh, zh_at, lambda t: core_parts.at[x, zh, r], lambda s: core_parts.at[x, s, r]
    )
    core_row = Exchange(
        sems, 2, 16, r, row_at, lambda t: core_parts.at[x, :, r], lambda s: core_parts.at[x, :, s]
    )
    core_x = RingOfFour(
        sems, 3, x, lambda t: core_parts.at[t], lambda t, h: core_parts.at[t, pl.ds(h * 2, 2)]
    )
    fac_row = Exchange(
        sems, 4, 16, r, row_at, lambda t: points.at[core, r, x], lambda s: points.at[core, s, x]
    )
    fac_x = RingOfFour(
        sems,
        5,
        x,
        lambda t: points.at[core, :, t],
        lambda t, h: points.at[core, pl.ds(h * 8, 8), t],
    )
    fac_swap = Swap(sems, 6, core, points.at[core], lambda s: points.at[s])
    hh_row = Exchange(
        sems,
        7,
        16,
        r,
        row_at,
        lambda t: rows.at[core, x, r, :, lanes],
        lambda s: rows.at[core, x, s, :, lanes],
    )

    def lanes_of(t):
        return pl.ds(pl.multiple_of(t * 128, 128), 128)

    hh_zh = Exchange(
        sems,
        8,
        4,
        zh,
        zh_at,
        lambda t: rows.at[core, x, :, :, lanes],
        lambda s: rows.at[core, x, :, :, lanes_of(s)],
    )
    hh_x = RingOfFour(
        sems, 9, x, lambda t: rows.at[core, t], lambda t, h: rows.at[core, t, pl.ds(h * 8, 8)]
    )
    hh_swap = Swap(sems, 10, core, rows.at[core], lambda s: rows.at[s])
    amp0_row = Exchange(sems, 11, 16, r, row_at, lambda t: own0.at[t], lambda s: in0.at[s])
    amp1_col = Exchange(sems, 12, 16, xz, col_at, lambda t: own1.at[t], lambda s: in1.at[s])
    amp0_col = Exchange(sems, 13, 16, xz, col_at, lambda t: mid0.at[t], lambda s: fin0.at[s])
    amp1_row = Exchange(sems, 14, 16, r, row_at, lambda t: mid1.at[t], lambda s: fin1.at[s])
    amp_swap = Swap(sems, 15, core, whole.at[core], lambda s: whole.at[s])
    lad_swap = Swap(sems, 16, core, give, lambda s: take)
    lad0_col = Exchange(sems, 17, 16, xz, col_at, lambda t: lad0.at[t], lambda s: got0.at[s])
    lad1_row = Exchange(sems, 18, 16, r, row_at, lambda t: lad1.at[t], lambda s: got1.at[s])
    lad0_row = Exchange(sems, 19, 16, r, row_at, lambda t: turn0.at[t], lambda s: back0.at[s])
    lad1_col = Exchange(sems, 20, 16, xz, col_at, lambda t: turn1.at[t], lambda s: back1.at[s])

    core_zh.start()

    fetch.wait()
    own_f32 = coupled
    own_f32[...] = jnp.zeros((256, 512), F32)

    def pick(k, carry):
        hit = owner[...] == iota((256, 512), 1) + k * 512
        own_f32[...] += nn(
            hit.astype(F32).astype(BF), amp[pl.ds(pl.multiple_of(k * 512, 512), 512), :]
        )
        return carry

    lax.fori_loop(0, 8, pick, 0)
    own[...] = own_f32[...].astype(BF)
    own0[...] = own[:, :256].reshape(16, 16, 256)
    own1[...] = nn(swap, own[:, 256:]).astype(BF).reshape(16, 16, 256)
    amp0_row.start()
    amp1_col.start()
    in0[r] = own0[r]
    in1[xz] = own1[xz]

    for d, c in hops:
        piece_in(d, c).wait_recv()
    point = iota((16, 256), 0)
    tile16 = jnp.zeros((16, 256), F32)
    for a in range(4):
        for b in range(2):
            for j in range(2):
                tile16 = jnp.where(
                    point == a * 4 + b * 2 + j, pieces[a, b, pl.ds(j, 1), :], tile16
                )
    points[core, r, x] = tile16.astype(BF)
    fac_row.start()
    core_zh.wait_recv()
    core_row.start()
    hh_row.start()
    order = order_matrix()

    amp0_row.wait_recv()
    mid0[...] = nn(swap, in0[...].reshape(256, 256)).astype(BF).reshape(16, 16, 256)
    amp0_col.start()
    fin0[xz] = mid0[xz]
    amp1_col.wait_recv()
    mid1[...] = nn(swap, in1[...].reshape(256, 256)).astype(BF).reshape(16, 16, 256)
    amp1_row.start()
    fin1[r] = mid1[r]

    fac_row.wait_recv()
    fac_x.start()
    core_row.wait_recv()
    core_x.start()
    fac_x.forward()
    core_x.forward()
    hh_row.wait_recv()
    hh_zh.start()

    amp0_col.wait_recv()
    whole[core, :, :256] = fin0[...].reshape(256, 256)
    amp1_row.wait_recv()
    whole[core, :, 256:] = nn(swap, fin1[...].reshape(256, 256)).astype(BF)
    amp_swap.start()

    fac_x.wait_recv()
    fac_swap.start()
    hh_zh.wait_recv()
    hh_x.start()
    amp_swap.wait_recv()
    fac_swap.wait_recv()

    def all_points(h):
        return points[h].reshape(1024, 256)

    def my_points(h):
        return points[h, :, pl.ds(core * 2, 2)].reshape(512, 256)

    order0[...] = (nt(my_points(0), order[:, :256]) + nt(my_points(1), order[:, 256:])).astype(BF)
    order1[...] = (nt(order[:, :256], my_points(0)) + nt(order[:, 256:], my_points(1))).astype(BF)

    for h in range(4):
        at = pl.ds(h * 4, 4)
        got = nt(whole[...].reshape(512, 512)[:, :256], points[0, at].reshape(256, 256))
        got += nt(whole[...].reshape(512, 512)[:, 256:], points[1, at].reshape(256, 256))
        half[:, h * 256 : h * 256 + 256] = got.astype(BF)

    core_x.wait_recv()
    hh_x.forward()
    low = iota((256, 128), 1) < 64
    for t in range(8):
        even = core_parts[:, :, 2 * t].reshape(256, 128).astype(F32)
        odd = core_parts[:, :, 2 * t + 1].reshape(256, 128).astype(F32)
        first = jnp.where(low, even, pltpu.roll(odd, 64, 1))
        second = jnp.where(low, pltpu.roll(even, 64, 1), odd)
        core_block[:, 0, :, t * 128 : t * 128 + 128] = first.astype(BF).reshape(16, 16, 128)
        core_block[:, 1, :, t * 128 : t * 128 + 128] = second.astype(BF).reshape(16, 16, 128)

    for t in range(4):
        cols = slice(t * 256, t * 256 + 256)
        middle = nn(order0[...], half[:, cols])
        weighted = (core_block[:, :, :, cols].reshape(512, 256).astype(F32) * middle).astype(BF)
        back = nn(order1[...], weighted).astype(BF)
        at = pl.ds(t * 4, 4)
        for h in range(2):
            part = nn(back, points[h, at].reshape(256, 256))
            put = slice(h * 256, h * 256 + 256)
            if t == 0:
                ladder[:, put] = part
            else:
                ladder[:, put] += part

    give[...] = ladder[pl.ds(pl.multiple_of(other * 256, 256), 256), :].astype(BF)
    lad_swap.start()
    hh_x.wait_recv()
    hh_swap.start()
    lad_swap.wait_recv()
    mine = ladder[pl.ds(pl.multiple_of(core * 256, 256), 256), :] + take[...].astype(F32)
    mine = mine.astype(BF)
    lad0[...] = mine[:, :256].reshape(16, 16, 256)
    lad0_col.start()
    lad1[...] = nn(swap, mine[:, 256:]).astype(BF).reshape(16, 16, 256)
    lad1_row.start()
    got0[xz] = lad0[xz]
    got1[r] = lad1[r]

    hh_swap.wait_recv()
    coupled[...] = jnp.zeros((256, 512), F32)

    def couple(k, carry):
        coupled[...] += nn(
            rows[k // 4, k % 4].reshape(256, 512),
            amp[pl.ds(pl.multiple_of(k * 512, 512), 512), :],
        )
        return carry

    lad0_col.wait_recv()
    turn0[...] = nn(swap, got0[...].reshape(256, 256)).astype(BF).reshape(16, 16, 256)
    lad0_row.start()
    back0[r] = turn0[r]
    lad1_row.wait_recv()
    turn1[...] = nn(swap, got1[...].reshape(256, 256)).astype(BF).reshape(16, 16, 256)
    lad1_col.start()
    back1[xz] = turn1[xz]

    lax.fori_loop(0, 8, couple, 0)
    device = r * 32 + xz * 2 + core
    vir_mine = jnp.sum(
        jnp.where(iota((1, 512), 1) == device, vir[...], 0.0), axis=1, keepdims=True
    )
    orbital = iota((256, 64), 1)
    first_hit = (owner[...] // 64) == orbital
    second_hit = (owner[...] % 64) == orbital
    occ_first = jnp.sum(jnp.where(first_hit, occ[...], 0.0), axis=1, keepdims=True)
    occ_second = jnp.sum(jnp.where(second_hit, occ[...], 0.0), axis=1, keepdims=True)
    occ_pair = occ_first + occ_second

    def finish(cols, lad):
        denom = (vir_mine + vir[:, cols]) - occ_pair
        rest = integrals[:, cols].astype(F32) + coupled[:, cols] + lad.astype(F32)
        update = 0.4 * own[:, cols].astype(F32) + 0.6 * rest / denom
        out[:, cols] = update.astype(BF)

    lad0_row.wait_recv()
    finish(slice(0, 256), back0[...].reshape(256, 256))
    lad1_col.wait_recv()
    finish(slice(256, 512), nn(swap, back1[...].reshape(256, 256)))

    for d, c in hops:
        piece_out(d, c).wait_send()
    for move in (
        core_zh, core_row, core_x, fac_row, fac_x, fac_swap, hh_row, hh_zh, hh_x, hh_swap,
        amp0_row, amp1_col, amp0_col, amp1_row, amp_swap, lad_swap,
        lad0_col, lad1_row, lad0_row, lad1_col,
    ):
        move.wait_send()


def per_device(
    amplitudes, integrals, hh_coupling, thc_factor, thc_core, occ_energy, vir_energy, pair_owner
):
    vmem = pl.BlockSpec(memory_space=pltpu.VMEM)
    cube = pltpu.VMEM((16, 16, 256), BF)
    scratch = [
        pltpu.VMEM((4096, 512), BF),
        pltpu.VMEM((256, 512), BF),
        *[cube] * 8,
        pltpu.VMEM((2, 256, 512), BF),
        pltpu.VMEM((2, 2, 256), F32),
        pltpu.VMEM((4, 2, 2, 256), F32),
        pltpu.VMEM((2, 16, 4, 16, 256), BF),
        pltpu.VMEM((4, 4, 16, 16, 128), BF),
        pltpu.VMEM((16, 2, 16, 1024), BF),
        pltpu.VMEM((2, 4, 16, 16, 512), BF),
        pltpu.VMEM((512, 1024), BF),
        pltpu.VMEM((512, 512), BF),
        pltpu.VMEM((512, 512), BF),
        pltpu.VMEM((512, 512), F32),
        pltpu.VMEM((256, 512), BF),
        pltpu.VMEM((256, 512), BF),
        *[cube] * 8,
        pltpu.VMEM((256, 512), F32),
        pltpu.SemaphoreType.DMA,
        pltpu.SemaphoreType.DMA((N_EXCHANGES, 16)),
        pltpu.SemaphoreType.DMA((N_EXCHANGES, 16)),
    ]
    return pl.pallas_call(
        kernel,
        out_shape=jax.ShapeDtypeStruct((256, 512), BF),
        in_specs=[pl.BlockSpec(memory_space=pl.ANY)] + [vmem] * 7,
        out_specs=vmem,
        scratch_shapes=scratch,
        compiler_params=pltpu.CompilerParams(
            collective_id=0, has_side_effects=True, vmem_limit_bytes=48 * 1024 * 1024
        ),
    )(
        amplitudes,
        integrals,
        hh_coupling,
        thc_factor.T,
        thc_core,
        occ_energy.reshape(1, -1),
        vir_energy.reshape(1, -1),
        pair_owner.reshape(-1, 1),
    )


def solution(mesh):
    finer = Mesh(mesh.devices.reshape(2, 8, 4, 4, 2), AXES)
    wide = P(None, ROW + COL)
    in_specs = (wide, wide, P(ROW, None), wide, P(COL, ROW), P(), P(), P())
    return jax.shard_map(
        per_device, mesh=finer, in_specs=in_specs, out_specs=wide, check_vma=False
    )
```

```python
import jax
import jax.numpy as jnp
from jax import lax
from jax.experimental import pallas as pl
from jax.experimental.pallas import tpu as pltpu
from jax.sharding import Mesh
from jax.sharding import PartitionSpec as P

AXES = ("zl", "y", "x", "zh", "core")
ROW = ("zl", "y")
COL = ("x", "zh", "core")
BF = jnp.bfloat16
F32 = jnp.float32
N_MOVES = 51


def nt(a, b):
    return lax.dot_general(a, b, (((1,), (1,)), ((), ())), preferred_element_type=F32)


def nn(a, b):
    return jnp.dot(a, b, preferred_element_type=F32)


def iota(shape, dim):
    return lax.broadcasted_iota(jnp.int32, shape, dim)


def swap_matrix():
    i, j = iota((256, 256), 0), iota((256, 256), 1)
    return (j == (i % 16) * 16 + i // 16).astype(F32).astype(BF)


def order_matrix():
    p, c = iota((512, 512), 0), iota((512, 512), 1)
    return (c == (p % 16) * 32 + ((p // 16) % 16) * 2 + p // 256).astype(F32).astype(BF)


def remote(src, dst, sems, slot, where):
    return pltpu.make_async_remote_copy(
        src_ref=src,
        dst_ref=dst,
        send_sem=sems[0].at[slot],
        recv_sem=sems[1].at[slot],
        device_id=where,
        device_id_type=pl.DeviceIdType.MESH,
    )


class Exchange:
    def __init__(self, sems, slot, count, me, where, src, dst, rest):
        self.sems, self.slot, self.count, self.me = sems, slot, count, me
        self.where, self.src, self.dst, self.rest = where, src, dst, rest

    def start(self):
        def step(d, carry):
            to = lax.rem(self.me + d, self.count)
            remote(
                self.src(to), self.dst(self.me), self.sems, self.slot, self.where(to)
            ).start()
            return carry

        lax.fori_loop(1, self.count, step, 0)

    def everything(self):
        to = lax.rem(self.me + 1, self.count)
        return remote(self.rest, self.rest, self.sems, self.slot, self.where(to))

    def wait_recv(self):
        self.everything().wait_recv()

    def wait_send(self):
        self.everything().wait_send()


class RingOfFour:
    def __init__(self, sems, slot, me, block, half):
        self.sems, self.slot = sems, slot
        self.me, self.right, self.across, self.left = (lax.rem(me + d, 4) for d in range(4))
        self.block, self.half = block, half

    def copy(self, part, ref, to):
        return remote(ref, ref, self.sems, self.slot + part, {"x": to})

    def start(self):
        self.copy(0, self.block(self.me), self.right).start()
        self.copy(1, self.block(self.me), self.left).start()

    def forward(self):
        self.copy(0, self.block(self.left), self.right).wait_recv()
        self.copy(2, self.half(self.left, 0), self.right).start()
        self.copy(1, self.block(self.right), self.left).wait_recv()
        self.copy(3, self.half(self.right, 1), self.left).start()

    def wait_recv(self):
        self.copy(2, self.half(self.across, 0), self.right).wait_recv()
        self.copy(3, self.half(self.across, 1), self.left).wait_recv()

    def wait_send(self):
        self.copy(0, self.block(self.me), self.right).wait_send()
        self.copy(1, self.block(self.me), self.left).wait_send()
        self.copy(2, self.half(self.left, 0), self.right).wait_send()
        self.copy(3, self.half(self.right, 1), self.left).wait_send()


class Swap:
    def __init__(self, sems, slot, core, src, dst):
        self.sems, self.slot, self.core = sems, slot, core
        self.src, self.dst = src, dst

    def copy(self, place):
        return remote(
            self.src, self.dst(place), self.sems, self.slot, {"core": 1 - self.core}
        )

    def start(self):
        self.copy(self.core).start()

    def wait_recv(self):
        self.copy(1 - self.core).wait_recv()

    def wait_send(self):
        self.copy(self.core).wait_send()


def kernel(
    amp_hbm, integrals_hbm, hh_hbm, factor_hbm, core_hbm, occ_hbm, vir_hbm, owner_hbm, out_hbm,
    amp, integrals, hh, factor, core_in, occ, vir, owner_row, out,
    own, own0, own1, in0, in1, mid0, mid1, fin0, fin1, whole,
    chunk, pieces, points, core_parts, rows, half, order0, order1, middle, weighted,
    give, take, lad0, lad1, got0, got1, turn0, turn1, back0, back1,
    coupled, in_sems, out_sems, send_sems, recv_sems,
):
    zl, y, x, zh, core = (lax.axis_index(a) for a in AXES)
    r, xz = zl * 8 + y, x * 4 + zh
    other = 1 - core
    sems = (send_sems, recv_sems)
    MESH = pl.DeviceIdType.MESH

    def row_at(t):
        return {"zl": t // 8, "y": t % 8}

    def col_at(t):
        return {"x": t // 4, "zh": t % 4}

    fetches = [
        pltpu.make_async_copy(src, dst, in_sems.at[k])
        for k, (src, dst) in enumerate(
            (
                (factor_hbm, factor),
                (core_hbm, core_in),
                (hh_hbm, hh),
                (owner_hbm, owner_row),
                (amp_hbm, amp),
                (occ_hbm, occ),
                (vir_hbm, vir),
                (integrals_hbm, integrals),
            )
        )
    ]
    for fetch in fetches[:4]:
        fetch.start()

    barrier = pltpu.get_barrier_semaphore()

    def greet(d, carry):
        pl.semaphore_signal(
            barrier, inc=1, device_id=row_at(lax.rem(r + d, 16)), device_id_type=MESH
        )
        pl.semaphore_signal(
            barrier, inc=1, device_id=col_at(lax.rem(xz + d, 16)), device_id_type=MESH
        )
        return carry

    lax.fori_loop(1, 16, greet, 0)
    for d in range(4):
        pl.semaphore_signal(
            barrier,
            inc=1,
            device_id={"zh": lax.rem(zh + d, 4), "core": other},
            device_id_type=MESH,
        )
    for fetch in fetches[4:]:
        fetch.start()

    swap = swap_matrix()
    for fetch in fetches[:4]:
        fetch.wait()
    for k in range(2):
        chunk[k] = factor[:, k * 256 : k * 256 + 256].astype(F32)
    pieces[zh, core] = chunk[core]
    core_parts[x, zh, r] = jnp.concatenate(
        [core_in[0:16, :], core_in[16:32, :]], axis=1
    ).astype(BF)
    rows[core, x, r] = hh[:, pl.ds(pl.multiple_of((core * 4 + x) * 512, 512), 512)]
    owner = jnp.sum(
        jnp.where(iota((256, 256), 0) == iota((256, 256), 1), owner_row[...], 0),
        axis=1,
        keepdims=True,
    )

    fetches[4].wait()
    coupled[...] = jnp.zeros((256, 512), F32)

    def pick(k, carry):
        hit = owner == iota((256, 512), 1) + k * 512
        coupled[...] += nn(
            hit.astype(F32).astype(BF), amp[pl.ds(pl.multiple_of(k * 512, 512), 512), :]
        )
        return carry

    lax.fori_loop(0, 8, pick, 0)
    own[...] = coupled[...].astype(BF)
    own0[...] = own[:, :256].reshape(16, 16, 256)
    own1[...] = nn(swap, own[:, 256:]).astype(BF).reshape(16, 16, 256)
    in0[r] = own0[r]
    in1[xz] = own1[xz]

    first15 = pl.ds(0, 15)

    def row_exchange(slot, src, dst, rest):
        return Exchange(sems, slot, 16, r, row_at, src, dst, rest)

    def col_exchange(slot, src, dst, rest):
        return Exchange(sems, slot, 16, xz, col_at, src, dst, rest)

    def block_exchange(make, slot, src, dst):
        return make(slot, lambda t: src.at[t], lambda s: dst.at[s], dst.at[first15])

    amp0_row = block_exchange(row_exchange, 0, own0, in0)
    amp1_col = block_exchange(col_exchange, 1, own1, in1)
    amp0_col = block_exchange(col_exchange, 2, mid0, fin0)
    amp1_row = block_exchange(row_exchange, 3, mid1, fin1)
    lad0_col = block_exchange(col_exchange, 4, lad0, got0)
    lad1_row = block_exchange(row_exchange, 5, lad1, got1)
    lad0_row = block_exchange(row_exchange, 6, turn0, back0)
    lad1_col = block_exchange(col_exchange, 7, turn1, back1)
    core_row = row_exchange(
        8,
        lambda t: core_parts.at[x, zh, r],
        lambda s: core_parts.at[x, zh, s],
        core_parts.at[x, zh, first15],
    )
    fac_row = row_exchange(
        9,
        lambda t: points.at[core, r, x],
        lambda s: points.at[core, s, x],
        points.at[core, first15, x],
    )
    hh_row = row_exchange(
        10,
        lambda t: rows.at[core, x, r],
        lambda s: rows.at[core, x, s],
        rows.at[core, x, first15],
    )
    fac_swap = Swap(sems, 11, core, points.at[core], lambda s: points.at[s])
    hh_swap = Swap(sems, 12, core, rows.at[core], lambda s: rows.at[s])
    amp_swap = Swap(sems, 13, core, whole.at[core], lambda s: whole.at[s])
    lad_swap = Swap(sems, 14, core, give, lambda s: take)
    fac_x = RingOfFour(
        sems,
        15,
        x,
        lambda t: points.at[core, :, t],
        lambda t, h: points.at[core, pl.ds(h * 8, 8), t],
    )
    hh_x = RingOfFour(
        sems, 19, x, lambda t: rows.at[core, t], lambda t, h: rows.at[core, t, pl.ds(h * 8, 8)]
    )

    def core_ring(d):
        z = lax.rem(zh + 4 - d, 4)
        return RingOfFour(
            sems,
            23 + 4 * d,
            x,
            lambda t: core_parts.at[t, z],
            lambda t, h: core_parts.at[t, z, pl.ds(h * 8, 8)],
        )

    core_rings = [core_ring(d) for d in range(4)]

    def core_zh(d, place):
        part = core_parts.at[x, place]
        return remote(part, part, sems, 39 + d, {"zh": lax.rem(zh + d, 4)})

    def core_zh_in(d):
        return core_zh(d, lax.rem(zh + 4 - d, 4))

    def piece(d, c, to_zh, to_core, slot_zh, slot_core):
        return remote(
            chunk.at[to_core],
            pieces.at[slot_zh, slot_core],
            sems,
            43 + d * 2 + c,
            {"zh": to_zh, "core": to_core},
        )

    hops = [(d, c) for d in range(4) for c in range(2) if d or c]

    def piece_out(d, c):
        return piece(d, c, lax.rem(zh + d, 4), core if c == 0 else other, zh, core)

    def piece_in(d, c):
        from_zh, from_core = lax.rem(zh + 4 - d, 4), core if c == 0 else other
        return piece(d, c, from_zh, from_core, from_zh, from_core)

    pl.semaphore_wait(barrier, 34)
    for d, c in hops:
        piece_out(d, c).start()
    core_row.start()
    amp0_row.start()
    amp1_col.start()
    order = order_matrix()

    for d, c in hops:
        piece_in(d, c).wait_recv()
    point = iota((16, 256), 0)
    tile16 = jnp.zeros((16, 256), F32)
    for a in range(4):
        for b in range(2):
            for j in range(2):
                tile16 = jnp.where(
                    point == a * 4 + b * 2 + j, pieces[a, b, pl.ds(j, 1), :], tile16
                )
    points[core, r, x] = tile16.astype(BF)
    fac_row.start()

    core_row.wait_recv()
    for d in (1, 3, 2):
        core_zh(d, zh).start()
    core_rings[0].start()

    amp0_row.wait_recv()
    mid0[...] = nn(swap, in0[...].reshape(256, 256)).astype(BF).reshape(16, 16, 256)
    amp0_col.start()
    fin0[xz] = mid0[xz]
    amp1_col.wait_recv()
    mid1[...] = nn(swap, in1[...].reshape(256, 256)).astype(BF).reshape(16, 16, 256)
    amp1_row.start()
    fin1[r] = mid1[r]

    fac_row.wait_recv()
    fac_x.start()
    hh_row.start()
    core_zh_in(1).wait_recv()
    core_rings[1].start()
    core_zh_in(3).wait_recv()
    core_rings[3].start()
    fac_x.forward()
    core_zh_in(2).wait_recv()
    core_rings[2].start()

    amp0_col.wait_recv()
    whole[core, :, :256] = fin0[...].reshape(256, 256)
    amp1_row.wait_recv()
    whole[core, :, 256:] = nn(swap, fin1[...].reshape(256, 256)).astype(BF)
    amp_swap.start()

    core_rings[0].forward()
    core_rings[1].forward()
    fac_x.wait_recv()
    fac_swap.start()
    core_rings[3].forward()
    core_rings[2].forward()
    hh_row.wait_recv()
    hh_x.start()
    amp_swap.wait_recv()
    fac_swap.wait_recv()

    def my_points(h):
        return points[h, :, pl.ds(core * 2, 2)].reshape(512, 256)

    for h in range(4):
        at = pl.ds(h * 4, 4)
        got = nt(whole[...].reshape(512, 512)[:, :256], points[0, at].reshape(256, 256))
        got += nt(whole[...].reshape(512, 512)[:, 256:], points[1, at].reshape(256, 256))
        half[:, h * 256 : h * 256 + 256] = got.astype(BF)
    order0[...] = (nt(my_points(0), order[:, :256]) + nt(my_points(1), order[:, 256:])).astype(BF)
    order1[...] = (nt(order[:, :256], my_points(0)) + nt(order[:, 256:], my_points(1))).astype(BF)
    for t in range(4):
        cols = slice(t * 256, t * 256 + 256)
        middle[:, :, :, cols] = nn(order0[...], half[:, cols]).reshape(16, 2, 16, 256)

    low = iota((64, 128), 1) < 64

    def weigh(block):
        at = pl.ds(block * 4, 4)
        for t in range(8):
            cols = slice(t * 128, t * 128 + 128)
            even = core_parts[block, :, 2 * t].reshape(64, 128).astype(F32)
            odd = core_parts[block, :, 2 * t + 1].reshape(64, 128).astype(F32)
            top = jnp.where(low, even, pltpu.roll(odd, 64, 1)).reshape(4, 16, 128)
            bottom = jnp.where(low, pltpu.roll(even, 64, 1), odd).reshape(4, 16, 128)
            weighted[at, 0, :, cols] = (top * middle[at, 0, :, cols]).astype(BF)
            weighted[at, 1, :, cols] = (bottom * middle[at, 1, :, cols]).astype(BF)

    def weigh_near(i, carry):
        weigh(lax.rem(x + i + i // 2, 4))
        return carry

    lax.fori_loop(0, 3, weigh_near, 0)
    for ring in core_rings:
        ring.wait_recv()
    weigh(lax.rem(x + 2, 4))

    def contract(side):
        at = pl.ds(pl.multiple_of(side * 256, 256), 256)
        back = nn(order1[at, :], weighted[...].reshape(512, 1024)).astype(BF)
        return [nn(back, points[h].reshape(1024, 256)) for h in range(2)]

    give0, give1 = contract(other)
    give[:, :256] = give0.astype(BF)
    give[:, 256:] = give1.astype(BF)
    lad_swap.start()
    mine0, mine1 = contract(core)
    hh_x.forward()
    lad_swap.wait_recv()
    lad0[...] = (mine0 + take[:, :256].astype(F32)).astype(BF).reshape(16, 16, 256)
    lad0_col.start()
    mine1 = (mine1 + take[:, 256:].astype(F32)).astype(BF)
    lad1[...] = nn(swap, mine1).astype(BF).reshape(16, 16, 256)
    lad1_row.start()
    got0[xz] = lad0[xz]
    got1[r] = lad1[r]
    hh_x.wait_recv()
    hh_swap.start()

    lad0_col.wait_recv()
    turn0[...] = nn(swap, got0[...].reshape(256, 256)).astype(BF).reshape(16, 16, 256)
    lad0_row.start()
    back0[r] = turn0[r]
    lad1_row.wait_recv()
    turn1[...] = nn(swap, got1[...].reshape(256, 256)).astype(BF).reshape(16, 16, 256)
    lad1_col.start()
    back1[xz] = turn1[xz]

    hh_swap.wait_recv()
    coupled[...] = jnp.zeros((256, 512), F32)

    def couple(k, carry):
        coupled[...] += nn(
            rows[k // 4, k % 4].reshape(256, 512),
            amp[pl.ds(pl.multiple_of(k * 512, 512), 512), :],
        )
        return carry

    lax.fori_loop(0, 8, couple, 0)
    for fetch in fetches[5:]:
        fetch.wait()
    device = r * 32 + xz * 2 + core
    vir_mine = jnp.sum(
        jnp.where(iota((1, 512), 1) == device, vir[...], 0.0), axis=1, keepdims=True
    )
    orbital = iota((256, 64), 1)
    first_hit = (owner // 64) == orbital
    second_hit = (owner % 64) == orbital
    occ_first = jnp.sum(jnp.where(first_hit, occ[...], 0.0), axis=1, keepdims=True)
    occ_second = jnp.sum(jnp.where(second_hit, occ[...], 0.0), axis=1, keepdims=True)
    occ_pair = occ_first + occ_second
    coupled[...] += integrals[...].astype(F32)

    def finish(k, lad):
        cols = slice(k * 256, k * 256 + 256)
        denom = (vir_mine + vir[:, cols]) - occ_pair
        rest = coupled[:, cols] + lad.astype(F32)
        update = 0.4 * own[:, cols].astype(F32) + 0.6 * rest / denom
        out[:, cols] = update.astype(BF)
        done = pltpu.make_async_copy(out.at[:, cols], out_hbm.at[:, cols], out_sems.at[k])
        done.start()
        return done

    lad0_row.wait_recv()
    done0 = finish(0, back0[...].reshape(256, 256))
    lad1_col.wait_recv()
    done1 = finish(1, nn(swap, back1[...].reshape(256, 256)))

    for d, c in hops:
        piece_out(d, c).wait_send()
    for d in (1, 2, 3):
        core_zh(d, zh).wait_send()
    for move in (
        core_row, *core_rings, fac_row, fac_x, fac_swap, hh_row, hh_x, hh_swap,
        amp0_row, amp1_col, amp0_col, amp1_row, amp_swap, lad_swap,
        lad0_col, lad1_row, lad0_row, lad1_col,
    ):
        move.wait_send()
    done0.wait()
    done1.wait()


def per_device(
    amplitudes, integrals, hh_coupling, thc_factor, thc_core, occ_energy, vir_energy, pair_owner
):
    cube = pltpu.VMEM((16, 16, 256), BF)
    scratch = [
        pltpu.VMEM((4096, 512), BF),
        pltpu.VMEM((256, 512), BF),
        pltpu.VMEM((16, 4096), BF),
        pltpu.VMEM((2, 512), BF),
        pltpu.VMEM((32, 64), F32),
        pltpu.VMEM((1, 64), F32),
        pltpu.VMEM((1, 512), F32),
        pltpu.VMEM((1, 256), jnp.int32),
        pltpu.VMEM((256, 512), BF),
        pltpu.VMEM((256, 512), BF),
        *[cube] * 8,
        pltpu.VMEM((2, 256, 512), BF),
        pltpu.VMEM((2, 2, 256), F32),
        pltpu.VMEM((4, 2, 2, 256), F32),
        pltpu.VMEM((2, 16, 4, 16, 256), BF),
        pltpu.VMEM((4, 4, 16, 16, 128), BF),
        pltpu.VMEM((2, 4, 16, 16, 512), BF),
        pltpu.VMEM((512, 1024), BF),
        pltpu.VMEM((512, 512), BF),
        pltpu.VMEM((512, 512), BF),
        pltpu.VMEM((16, 2, 16, 1024), F32),
        pltpu.VMEM((16, 2, 16, 1024), BF),
        pltpu.VMEM((256, 512), BF),
        pltpu.VMEM((256, 512), BF),
        *[cube] * 8,
        pltpu.VMEM((256, 512), F32),
        pltpu.SemaphoreType.DMA((8,)),
        pltpu.SemaphoreType.DMA((2,)),
        pltpu.SemaphoreType.DMA((N_MOVES,)),
        pltpu.SemaphoreType.DMA((N_MOVES,)),
    ]
    return pl.pallas_call(
        kernel,
        out_shape=jax.ShapeDtypeStruct((256, 512), BF),
        in_specs=[pl.BlockSpec(memory_space=pltpu.HBM)] * 8,
        out_specs=pl.BlockSpec(memory_space=pltpu.HBM),
        scratch_shapes=scratch,
        compiler_params=pltpu.CompilerParams(
            collective_id=0, has_side_effects=True, vmem_limit_bytes=67043328
        ),
    )(
        amplitudes,
        integrals,
        hh_coupling,
        thc_factor.T,
        thc_core,
        occ_energy.reshape(1, -1),
        vir_energy.reshape(1, -1),
        pair_owner.reshape(1, -1),
    )


def solution(mesh):
    finer = Mesh(mesh.devices.reshape(2, 8, 4, 4, 2), AXES)
    wide = P(None, ROW + COL)
    in_specs = (wide, wide, P(ROW, None), wide, P(COL, ROW), P(), P(), P())
    return jax.shard_map(
        per_device, mesh=finer, in_specs=in_specs, out_specs=wide, check_vma=False
    )
```

```python
import jax
import jax.numpy as jnp
from jax import lax
from jax.experimental import pallas as pl
from jax.experimental.pallas import tpu as pltpu
from jax.sharding import Mesh
from jax.sharding import PartitionSpec as P

AXES = ("zl", "y", "x", "zh", "core")
ROW = ("zl", "y")
COL = ("x", "zh", "core")
BF = jnp.bfloat16
F32 = jnp.float32
N_MOVES = 58


def nt(a, b):
    return lax.dot_general(a, b, (((1,), (1,)), ((), ())), preferred_element_type=F32)


def nn(a, b):
    return jnp.dot(a, b, preferred_element_type=F32)


def iota(shape, dim):
    return lax.broadcasted_iota(jnp.int32, shape, dim)


def swap_matrix():
    i, j = iota((256, 256), 0), iota((256, 256), 1)
    return (j == (i % 16) * 16 + i // 16).astype(F32).astype(BF)


def order_matrix():
    p, c = iota((512, 512), 0), iota((512, 512), 1)
    return (c == (p % 16) * 32 + ((p // 16) % 16) * 2 + p // 256).astype(F32).astype(BF)


def remote(src, dst, sems, slot, where):
    return pltpu.make_async_remote_copy(
        src_ref=src,
        dst_ref=dst,
        send_sem=sems[0].at[slot],
        recv_sem=sems[1].at[slot],
        device_id=where,
        device_id_type=pl.DeviceIdType.MESH,
    )


class Single:
    def __init__(self, outgoing, incoming):
        self.outgoing, self.incoming = outgoing, incoming

    def start(self):
        self.outgoing().start()

    def wait_recv(self):
        self.incoming().wait_recv()

    def wait_send(self):
        self.outgoing().wait_send()


class Exchange:
    def __init__(self, sems, slot, count, me, where, src, dst, rest):
        self.sems, self.slot, self.count, self.me = sems, slot, count, me
        self.where, self.src, self.dst, self.rest = where, src, dst, rest

    def start(self):
        def step(d, carry):
            to = lax.rem(self.me + d, self.count)
            remote(
                self.src(to), self.dst(self.me), self.sems, self.slot, self.where(to)
            ).start()
            return carry

        lax.fori_loop(1, self.count, step, 0)

    def everything(self):
        to = lax.rem(self.me + 1, self.count)
        return remote(self.rest, self.rest, self.sems, self.slot, self.where(to))

    def wait_recv(self):
        self.everything().wait_recv()

    def wait_send(self):
        self.everything().wait_send()


class RingOfFour:
    def __init__(self, sems, slot, me, block, half):
        self.sems, self.slot = sems, slot
        self.me, self.right, self.across, self.left = (lax.rem(me + d, 4) for d in range(4))
        self.block, self.half = block, half

    def copy(self, part, ref, to):
        return remote(ref, ref, self.sems, self.slot + part, {"x": to})

    def start(self):
        self.copy(0, self.block(self.me), self.right).start()
        self.copy(1, self.block(self.me), self.left).start()

    def forward(self):
        self.copy(0, self.block(self.left), self.right).wait_recv()
        self.copy(2, self.half(self.left, 0), self.right).start()
        self.copy(1, self.block(self.right), self.left).wait_recv()
        self.copy(3, self.half(self.right, 1), self.left).start()

    def wait_recv(self):
        self.copy(2, self.half(self.across, 0), self.right).wait_recv()
        self.copy(3, self.half(self.across, 1), self.left).wait_recv()

    def wait_send(self):
        self.copy(0, self.block(self.me), self.right).wait_send()
        self.copy(1, self.block(self.me), self.left).wait_send()
        self.copy(2, self.half(self.left, 0), self.right).wait_send()
        self.copy(3, self.half(self.right, 1), self.left).wait_send()


class Swap:
    def __init__(self, sems, slot, core, src, dst):
        self.sems, self.slot, self.core = sems, slot, core
        self.src, self.dst = src, dst

    def copy(self, place):
        return remote(
            self.src, self.dst(place), self.sems, self.slot, {"core": 1 - self.core}
        )

    def start(self):
        self.copy(self.core).start()

    def wait_recv(self):
        self.copy(1 - self.core).wait_recv()

    def wait_send(self):
        self.copy(self.core).wait_send()


def kernel(
    amp_hbm, integrals_hbm, hh_hbm, factor_hbm, core_hbm, occ_hbm, vir_hbm, owner_hbm, out,
    amp, integrals, hh, factor, core_in, occ, vir, owner_row,
    own, own0, own1, in0, in1, mid0, mid1, fin0, fin1, whole,
    chunk, pieces, points, core_parts, rows, half, order, order0, order1, half_part, part0, part1, middle, weighted,
    give, take, lad0, lad1, got0, got1, turn0, turn1, back0, back1,
    coupled, in_sems, send_sems, recv_sems,
):
    zl, y, x, zh, core = (lax.axis_index(a) for a in AXES)
    r, xz = zl * 8 + y, x * 4 + zh
    other = 1 - core
    sems = (send_sems, recv_sems)
    MESH = pl.DeviceIdType.MESH

    def row_at(t):
        return {"zl": t // 8, "y": t % 8}

    def col_at(t):
        return {"x": t // 4, "zh": t % 4}

    fetches = [
        pltpu.make_async_copy(src, dst, in_sems.at[k])
        for k, (src, dst) in enumerate(
            (
                (factor_hbm, factor),
                (core_hbm, core_in),
                (owner_hbm, owner_row),
                (hh_hbm, hh),
                (occ_hbm, occ),
                (vir_hbm, vir),
                (integrals_hbm, integrals),
            )
        )
    ]
    for fetch in fetches[:3]:
        fetch.start()

    def eighth(k):
        at = pl.ds(pl.multiple_of(k * 512, 512), 512)
        return pltpu.make_async_copy(amp_hbm.at[at], amp.at[at], in_sems.at[7 + k])

    barrier = pltpu.get_barrier_semaphore()

    def greet(d, carry):
        pl.semaphore_signal(
            barrier, inc=1, device_id=row_at(lax.rem(r + d, 16)), device_id_type=MESH
        )
        pl.semaphore_signal(
            barrier, inc=1, device_id=col_at(lax.rem(xz + d, 16)), device_id_type=MESH
        )
        return carry

    lax.fori_loop(1, 16, greet, 0)
    for d in range(4):
        pl.semaphore_signal(
            barrier,
            inc=1,
            device_id={"zh": lax.rem(zh + d, 4), "core": other},
            device_id_type=MESH,
        )
    for k in range(8):
        eighth(k).start()
    for fetch in fetches[3:]:
        fetch.start()

    swap = swap_matrix()
    for fetch in fetches[:3]:
        fetch.wait()
    for k in range(2):
        chunk[k] = factor[:, k * 256 : k * 256 + 256].astype(F32)
    pieces[zh, core] = chunk[core]
    core_parts[x, zh, r] = jnp.concatenate(
        [core_in[0:16, :], core_in[16:32, :]], axis=1
    ).astype(BF)
    owner = jnp.sum(
        jnp.where(iota((256, 256), 0) == iota((256, 256), 1), owner_row[...], 0),
        axis=1,
        keepdims=True,
    )

    coupled[...] = jnp.zeros((256, 512), F32)

    def pick(k, carry):
        eighth(k).wait()
        hit = owner == iota((256, 512), 1) + k * 512
        coupled[...] += nn(
            hit.astype(F32).astype(BF), amp[pl.ds(pl.multiple_of(k * 512, 512), 512), :]
        )
        return carry

    lax.fori_loop(0, 5, pick, 0)

    first15 = pl.ds(0, 15)

    def row_exchange(slot, src, dst, rest):
        return Exchange(sems, slot, 16, r, row_at, src, dst, rest)

    def col_exchange(slot, src, dst, rest):
        return Exchange(sems, slot, 16, xz, col_at, src, dst, rest)

    def block_exchange(make, slot, src, dst):
        return make(slot, lambda t: src.at[t], lambda s: dst.at[s], dst.at[first15])

    amp0_row = block_exchange(row_exchange, 0, own0, in0)
    amp1_col = block_exchange(col_exchange, 1, own1, in1)
    amp0_col = block_exchange(col_exchange, 2, mid0, fin0)
    amp1_row = block_exchange(row_exchange, 3, mid1, fin1)
    lad0_col = block_exchange(col_exchange, 4, lad0, got0)
    lad1_row = block_exchange(row_exchange, 5, lad1, got1)
    lad0_row = block_exchange(row_exchange, 6, turn0, back0)
    lad1_col = block_exchange(col_exchange, 7, turn1, back1)
    core_row = row_exchange(
        8,
        lambda t: core_parts.at[x, zh, r],
        lambda s: core_parts.at[x, zh, s],
        core_parts.at[x, zh, first15],
    )
    fac_row = row_exchange(
        9,
        lambda t: points.at[core, r, x],
        lambda s: points.at[core, s, x],
        points.at[core, first15, x],
    )
    hh_row = row_exchange(
        10,
        lambda t: rows.at[core, x, r],
        lambda s: rows.at[core, x, s],
        rows.at[core, x, first15],
    )

    def fac_part(slot, d):
        t = lax.rem(x + d, 4)
        return Swap(sems, slot, core, points.at[core, :, t], lambda s: points.at[s, :, t])

    def hh_part(slot, d):
        t = lax.rem(x + d, 4)
        return Swap(sems, slot, core, rows.at[core, t], lambda s: rows.at[s, t])

    fac_swaps = [fac_part(slot, d) for d, slot in enumerate((11, 51, 52, 53))]
    hh_swaps = [hh_part(slot, d) for d, slot in enumerate((12, 55, 56, 57))]
    amp_swap = Swap(sems, 13, core, whole.at[core], lambda s: whole.at[s])
    lad_swaps = [
        Swap(sems, slot, core, give.at[h], lambda s, h=h: take.at[h])
        for h, slot in enumerate((14, 54))
    ]
    fac_x = RingOfFour(
        sems,
        15,
        x,
        lambda t: points.at[core, :, t],
        lambda t, h: points.at[core, pl.ds(h * 8, 8), t],
    )
    hh_x = RingOfFour(
        sems, 19, x, lambda t: rows.at[core, t], lambda t, h: rows.at[core, t, pl.ds(h * 8, 8)]
    )

    def core_ring(d):
        z = lax.rem(zh + 4 - d, 4)
        return RingOfFour(
            sems,
            23 + 4 * d,
            x,
            lambda t: core_parts.at[t, z],
            lambda t, h: core_parts.at[t, z, pl.ds(h * 8, 8)],
        )

    core_rings = [core_ring(d) for d in range(4)]

    def core_step(d):
        def copy(place):
            part = core_parts.at[x, place]
            return remote(part, part, sems, 39 + d, {"zh": lax.rem(zh + d, 4)})

        return Single(lambda: copy(zh), lambda: copy(lax.rem(zh + 4 - d, 4)))

    core_zh = {d: core_step(d) for d in (1, 3, 2)}

    def piece_step(d, c):
        def copy(to_zh, to_core, slot_zh, slot_core):
            return remote(
                chunk.at[to_core],
                pieces.at[slot_zh, slot_core],
                sems,
                43 + d * 2 + c,
                {"zh": to_zh, "core": to_core},
            )

        peer = core if c == 0 else other
        source = lax.rem(zh + 4 - d, 4)
        return Single(
            lambda: copy(lax.rem(zh + d, 4), peer, zh, core),
            lambda: copy(source, peer, source, peer),
        )

    hops = [piece_step(d, c) for d in range(4) for c in range(2) if d or c]

    pl.semaphore_wait(barrier, 34)
    for hop in hops:
        hop.start()
    core_row.start()
    lax.fori_loop(5, 8, pick, 0)
    own[...] = coupled[...].astype(BF)
    own0[...] = own[:, :256].reshape(16, 16, 256)
    own1[...] = nn(swap, own[:, 256:]).astype(BF).reshape(16, 16, 256)
    amp0_row.start()
    amp1_col.start()
    in0[r] = own0[r]
    in1[xz] = own1[xz]
    fetches[3].wait()
    rows[core, x, r] = hh[:, pl.ds(pl.multiple_of((core * 4 + x) * 512, 512), 512)]
    order[...] = order_matrix()

    for hop in hops:
        hop.wait_recv()
    point = iota((16, 256), 0)
    tile16 = jnp.zeros((16, 256), F32)
    for a in range(4):
        for b in range(2):
            for j in range(2):
                tile16 = jnp.where(
                    point == a * 4 + b * 2 + j, pieces[a, b, pl.ds(j, 1), :], tile16
                )
    points[core, r, x] = tile16.astype(BF)
    fac_row.start()

    core_row.wait_recv()
    for step in core_zh.values():
        step.start()
    core_rings[0].start()

    amp0_row.wait_recv()
    mid0[...] = nn(swap, in0[...].reshape(256, 256)).astype(BF).reshape(16, 16, 256)
    amp0_col.start()
    fin0[xz] = mid0[xz]
    amp1_col.wait_recv()
    mid1[...] = nn(swap, in1[...].reshape(256, 256)).astype(BF).reshape(16, 16, 256)
    amp1_row.start()
    fin1[r] = mid1[r]

    fac_row.wait_recv()
    fac_x.start()
    fac_swaps[0].start()
    hh_row.start()
    core_zh[1].wait_recv()
    core_rings[1].start()
    core_zh[3].wait_recv()
    core_rings[3].start()
    fac_x.forward()
    fac_swaps[1].start()
    fac_swaps[3].start()
    core_zh[2].wait_recv()
    core_rings[2].start()

    amp0_col.wait_recv()
    whole[core, :, :256] = fin0[...].reshape(256, 256)
    amp1_row.wait_recv()
    whole[core, :, 256:] = nn(swap, fin1[...].reshape(256, 256)).astype(BF)
    amp_swap.start()

    def my_points(h):
        return points[h, :, pl.ds(core * 2, 2)].reshape(512, 256)

    def lanes_half(h):
        return pl.ds(pl.multiple_of(h * 256, 256), 256)

    def half_from(h, t):
        left = whole[:, :, lanes_half(h)].reshape(512, 256)
        return nt(left, points[h, pl.ds(t * 4, 4)].reshape(256, 256))

    core_rings[0].forward()
    core_rings[1].forward()
    fac_x.wait_recv()
    fac_swaps[2].start()
    core_rings[3].forward()
    amp_swap.wait_recv()

    for t in range(4):
        half_part[:, t * 256 : t * 256 + 256] = half_from(core, t)
    part0[...] = nt(my_points(core), order[:, lanes_half(core)])
    part1[...] = nt(order[:, lanes_half(core)], my_points(core))

    core_rings[2].forward()
    hh_row.wait_recv()
    hh_x.start()
    hh_swaps[0].start()
    for part in fac_swaps:
        part.wait_recv()

    for t in range(4):
        cols = slice(t * 256, t * 256 + 256)
        half[:, cols] = (half_part[:, cols] + half_from(other, t)).astype(BF)
    order0[...] = (part0[...] + nt(my_points(other), order[:, lanes_half(other)])).astype(BF)
    order1[...] = (part1[...] + nt(order[:, lanes_half(other)], my_points(other))).astype(BF)
    for t in range(4):
        cols = slice(t * 256, t * 256 + 256)
        middle[:, :, :, cols] = nn(order0[...], half[:, cols]).reshape(16, 2, 16, 256)

    low = iota((64, 128), 1) < 64

    def weigh(block):
        at = pl.ds(block * 4, 4)
        for t in range(8):
            cols = slice(t * 128, t * 128 + 128)
            even = core_parts[block, :, 2 * t].reshape(64, 128).astype(F32)
            odd = core_parts[block, :, 2 * t + 1].reshape(64, 128).astype(F32)
            top = jnp.where(low, even, pltpu.roll(odd, 64, 1)).reshape(4, 16, 128)
            bottom = jnp.where(low, pltpu.roll(even, 64, 1), odd).reshape(4, 16, 128)
            weighted[at, 0, :, cols] = (top * middle[at, 0, :, cols]).astype(BF)
            weighted[at, 1, :, cols] = (bottom * middle[at, 1, :, cols]).astype(BF)

    def weigh_near(i, carry):
        weigh(lax.rem(x + i + i // 2, 4))
        return carry

    lax.fori_loop(0, 3, weigh_near, 0)
    for ring in core_rings:
        ring.wait_recv()
    weigh(lax.rem(x + 2, 4))

    def back_of(side):
        at = pl.ds(pl.multiple_of(side * 256, 256), 256)
        return nn(order1[at, :], weighted[...].reshape(512, 1024)).astype(BF)

    def ladder_of(back, h):
        return nn(back, points[h].reshape(1024, 256))

    back = back_of(other)
    for h in range(2):
        give[h] = ladder_of(back, h).astype(BF)
        lad_swaps[h].start()
    back = back_of(core)
    mine = ladder_of(back, 0)
    lad_swaps[0].wait_recv()
    lad0[...] = (mine + take[0].astype(F32)).astype(BF).reshape(16, 16, 256)
    lad0_col.start()
    mine = ladder_of(back, 1)
    lad_swaps[1].wait_recv()
    mine = (mine + take[1].astype(F32)).astype(BF)
    lad1[...] = nn(swap, mine).astype(BF).reshape(16, 16, 256)
    lad1_row.start()
    hh_x.forward()
    hh_swaps[1].start()
    hh_swaps[3].start()
    got0[xz] = lad0[xz]
    got1[r] = lad1[r]

    lad0_col.wait_recv()
    turn0[...] = nn(swap, got0[...].reshape(256, 256)).astype(BF).reshape(16, 16, 256)
    lad0_row.start()
    back0[r] = turn0[r]
    lad1_row.wait_recv()
    turn1[...] = nn(swap, got1[...].reshape(256, 256)).astype(BF).reshape(16, 16, 256)
    lad1_col.start()
    back1[xz] = turn1[xz]

    hh_x.wait_recv()
    hh_swaps[2].start()
    for part in hh_swaps:
        part.wait_recv()
    coupled[...] = jnp.zeros((256, 512), F32)

    def couple(k, carry):
        coupled[...] += nn(
            rows[k // 4, k % 4].reshape(256, 512),
            amp[pl.ds(pl.multiple_of(k * 512, 512), 512), :],
        )
        return carry

    lax.fori_loop(0, 8, couple, 0)
    for fetch in fetches[4:]:
        fetch.wait()
    device = r * 32 + xz * 2 + core
    vir_mine = jnp.sum(
        jnp.where(iota((1, 512), 1) == device, vir[...], 0.0), axis=1, keepdims=True
    )
    orbital = iota((256, 64), 1)
    first_hit = (owner // 64) == orbital
    second_hit = (owner % 64) == orbital
    occ_first = jnp.sum(jnp.where(first_hit, occ[...], 0.0), axis=1, keepdims=True)
    occ_second = jnp.sum(jnp.where(second_hit, occ[...], 0.0), axis=1, keepdims=True)
    occ_pair = occ_first + occ_second
    coupled[...] += integrals[...].astype(F32)

    def finish(k, lad):
        cols = slice(k * 256, k * 256 + 256)
        denom = (vir_mine + vir[:, cols]) - occ_pair
        rest = coupled[:, cols] + lad.astype(F32)
        update = 0.4 * own[:, cols].astype(F32) + 0.6 * rest / denom
        out[:, cols] = update.astype(BF)

    lad0_row.wait_recv()
    finish(0, back0[...].reshape(256, 256))
    lad1_col.wait_recv()
    finish(1, nn(swap, back1[...].reshape(256, 256)))

    for move in (
        *hops, *core_zh.values(), core_row, *core_rings, fac_row, fac_x, *fac_swaps, hh_row, hh_x, *hh_swaps,
        amp0_row, amp1_col, amp0_col, amp1_row, amp_swap, *lad_swaps,
        lad0_col, lad1_row, lad0_row, lad1_col,
    ):
        move.wait_send()


def per_device(
    amplitudes, integrals, hh_coupling, thc_factor, thc_core, occ_energy, vir_energy, pair_owner
):
    cube = pltpu.VMEM((16, 16, 256), BF)
    scratch = [
        pltpu.VMEM((4096, 512), BF),
        pltpu.VMEM((256, 512), BF),
        pltpu.VMEM((16, 4096), BF),
        pltpu.VMEM((2, 512), BF),
        pltpu.VMEM((32, 64), F32),
        pltpu.VMEM((1, 64), F32),
        pltpu.VMEM((1, 512), F32),
        pltpu.VMEM((1, 256), jnp.int32),
        pltpu.VMEM((256, 512), BF),
        *[cube] * 8,
        pltpu.VMEM((2, 256, 512), BF),
        pltpu.VMEM((2, 2, 256), F32),
        pltpu.VMEM((4, 2, 2, 256), F32),
        pltpu.VMEM((2, 16, 4, 16, 256), BF),
        pltpu.VMEM((4, 4, 16, 16, 128), BF),
        pltpu.VMEM((2, 4, 16, 16, 512), BF),
        pltpu.VMEM((512, 1024), BF),
        pltpu.VMEM((512, 512), BF),
        pltpu.VMEM((512, 512), BF),
        pltpu.VMEM((512, 512), BF),
        pltpu.VMEM((512, 1024), F32),
        pltpu.VMEM((512, 512), F32),
        pltpu.VMEM((512, 512), F32),
        pltpu.VMEM((16, 2, 16, 1024), F32),
        pltpu.VMEM((16, 2, 16, 1024), BF),
        pltpu.VMEM((2, 256, 256), BF),
        pltpu.VMEM((2, 256, 256), BF),
        *[cube] * 8,
        pltpu.VMEM((256, 512), F32),
        pltpu.SemaphoreType.DMA((15,)),
        pltpu.SemaphoreType.DMA((N_MOVES,)),
        pltpu.SemaphoreType.DMA((N_MOVES,)),
    ]
    return pl.pallas_call(
        kernel,
        out_shape=jax.ShapeDtypeStruct((256, 512), BF),
        in_specs=[pl.BlockSpec(memory_space=pltpu.HBM)] * 8,
        out_specs=pl.BlockSpec(memory_space=pltpu.VMEM),
        scratch_shapes=scratch,
        compiler_params=pltpu.CompilerParams(
            collective_id=0, has_side_effects=True, vmem_limit_bytes=50000000
        ),
    )(
        *(
            pltpu.with_memory_space_constraint(operand, pltpu.HBM)
            for operand in (
                amplitudes,
                integrals,
                hh_coupling,
                thc_factor.T,
                thc_core,
                occ_energy.reshape(1, -1),
                vir_energy.reshape(1, -1),
                pair_owner.reshape(1, -1),
            )
        )
    )


def solution(mesh):
    finer = Mesh(mesh.devices.reshape(2, 8, 4, 4, 2), AXES)
    wide = P(None, ROW + COL)
    in_specs = (wide, wide, P(ROW, None), wide, P(COL, ROW), P(), P(), P())
    return jax.shard_map(
        per_device, mesh=finer, in_specs=in_specs, out_specs=wide, check_vma=False
    )
```

```python
import jax
import jax.numpy as jnp
from jax import lax
from jax.experimental import pallas as pl
from jax.experimental.pallas import tpu as pltpu
from jax.sharding import Mesh
from jax.sharding import PartitionSpec as P

AXES = ("zl", "y", "x", "zh", "core")
ROW = ("zl", "y")
COL = ("x", "zh", "core")
BF = jnp.bfloat16
F32 = jnp.float32
N_MOVES = 58


def nt(a, b):
    return lax.dot_general(a, b, (((1,), (1,)), ((), ())), preferred_element_type=F32)


def nn(a, b):
    return jnp.dot(a, b, preferred_element_type=F32)


def iota(shape, dim):
    return lax.broadcasted_iota(jnp.int32, shape, dim)


def swap_matrix():
    i, j = iota((256, 256), 0), iota((256, 256), 1)
    return (j == (i % 16) * 16 + i // 16).astype(F32).astype(BF)


def order_matrix():
    p, c = iota((512, 512), 0), iota((512, 512), 1)
    return (c == (p % 16) * 32 + ((p // 16) % 16) * 2 + p // 256).astype(F32).astype(BF)


def remote(src, dst, sems, slot, where):
    return pltpu.make_async_remote_copy(
        src_ref=src,
        dst_ref=dst,
        send_sem=sems[0].at[slot],
        recv_sem=sems[1].at[slot],
        device_id=where,
        device_id_type=pl.DeviceIdType.MESH,
    )


class Single:
    def __init__(self, outgoing, incoming):
        self.outgoing, self.incoming = outgoing, incoming

    def start(self):
        self.outgoing().start()

    def wait_recv(self):
        self.incoming().wait_recv()

    def wait_send(self):
        self.outgoing().wait_send()


class Exchange:
    def __init__(self, sems, slot, count, me, where, src, dst, rest):
        self.sems, self.slot, self.count, self.me = sems, slot, count, me
        self.where, self.src, self.dst, self.rest = where, src, dst, rest

    def start(self):
        def step(d, carry):
            to = lax.rem(self.me + d, self.count)
            remote(
                self.src(to), self.dst(self.me), self.sems, self.slot, self.where(to)
            ).start()
            return carry

        lax.fori_loop(1, self.count, step, 0)

    def everything(self):
        to = lax.rem(self.me + 1, self.count)
        return remote(self.rest, self.rest, self.sems, self.slot, self.where(to))

    def wait_recv(self):
        self.everything().wait_recv()

    def wait_send(self):
        self.everything().wait_send()


class RingOfFour:
    def __init__(self, sems, slot, me, block, half):
        self.sems, self.slot = sems, slot
        self.me, self.right, self.across, self.left = (lax.rem(me + d, 4) for d in range(4))
        self.block, self.half = block, half

    def copy(self, part, ref, to):
        return remote(ref, ref, self.sems, self.slot + part, {"x": to})

    def start(self):
        self.copy(0, self.block(self.me), self.right).start()
        self.copy(1, self.block(self.me), self.left).start()

    def forward(self):
        self.copy(0, self.block(self.left), self.right).wait_recv()
        self.copy(2, self.half(self.left, 0), self.right).start()
        self.copy(1, self.block(self.right), self.left).wait_recv()
        self.copy(3, self.half(self.right, 1), self.left).start()

    def wait_recv(self):
        self.copy(2, self.half(self.across, 0), self.right).wait_recv()
        self.copy(3, self.half(self.across, 1), self.left).wait_recv()

    def wait_send(self):
        self.copy(0, self.block(self.me), self.right).wait_send()
        self.copy(1, self.block(self.me), self.left).wait_send()
        self.copy(2, self.half(self.left, 0), self.right).wait_send()
        self.copy(3, self.half(self.right, 1), self.left).wait_send()


class Swap:
    def __init__(self, sems, slot, core, src, dst):
        self.sems, self.slot, self.core = sems, slot, core
        self.src, self.dst = src, dst

    def copy(self, place):
        return remote(
            self.src, self.dst(place), self.sems, self.slot, {"core": 1 - self.core}
        )

    def start(self):
        self.copy(self.core).start()

    def wait_recv(self):
        self.copy(1 - self.core).wait_recv()

    def wait_send(self):
        self.copy(self.core).wait_send()


def kernel(
    amp_hbm, integrals_hbm, hh_hbm, factor_hbm, core_hbm, occ_hbm, vir_hbm, owner_hbm, out,
    amp, integrals, hh, factor, core_in, occ, vir, owner_row,
    own, own0, own1, in0, in1, mid0, mid1, fin0, fin1, whole,
    chunk, pieces, points, core_parts, rows, half, order, order0, order1, half_part, part0, part1, middle, weighted,
    give, take, lad0, lad1, got0, got1, turn0, turn1, back0, back1,
    coupled, in_sems, send_sems, recv_sems,
):
    zl, y, x, zh, core = (lax.axis_index(a) for a in AXES)
    r, xz = zl * 8 + y, x * 4 + zh
    other = 1 - core
    sems = (send_sems, recv_sems)
    MESH = pl.DeviceIdType.MESH

    def row_at(t):
        return {"zl": t // 8, "y": t % 8}

    def col_at(t):
        return {"x": t // 4, "zh": t % 4}

    fetches = [
        pltpu.make_async_copy(src, dst, in_sems.at[k])
        for k, (src, dst) in enumerate(
            (
                (factor_hbm, factor),
                (core_hbm, core_in),
                (owner_hbm, owner_row),
                (hh_hbm, hh),
                (occ_hbm, occ),
                (vir_hbm, vir),
                (integrals_hbm, integrals),
            )
        )
    ]
    for fetch in fetches[:3]:
        fetch.start()

    def eighth(k):
        at = pl.ds(pl.multiple_of(k * 512, 512), 512)
        return pltpu.make_async_copy(amp_hbm.at[at], amp.at[at], in_sems.at[7 + k])

    barrier = pltpu.get_barrier_semaphore()

    def greet(d, carry):
        pl.semaphore_signal(
            barrier, inc=1, device_id=row_at(lax.rem(r + d, 16)), device_id_type=MESH
        )
        pl.semaphore_signal(
            barrier, inc=1, device_id=col_at(lax.rem(xz + d, 16)), device_id_type=MESH
        )
        return carry

    lax.fori_loop(1, 16, greet, 0)
    for d in range(4):
        pl.semaphore_signal(
            barrier,
            inc=1,
            device_id={"zh": lax.rem(zh + d, 4), "core": other},
            device_id_type=MESH,
        )
    for k in range(8):
        eighth(k).start()
    for fetch in fetches[3:]:
        fetch.start()

    swap = swap_matrix()
    for fetch in fetches[:3]:
        fetch.wait()
    for k in range(2):
        chunk[k] = factor[:, k * 256 : k * 256 + 256].astype(F32)
    pieces[zh, core] = chunk[core]
    core_parts[x, zh, r] = jnp.concatenate(
        [core_in[0:16, :], core_in[16:32, :]], axis=1
    ).astype(BF)
    owner = jnp.sum(
        jnp.where(iota((256, 256), 0) == iota((256, 256), 1), owner_row[...], 0),
        axis=1,
        keepdims=True,
    )

    coupled[...] = jnp.zeros((256, 512), F32)

    def pick(k, carry):
        eighth(k).wait()
        hit = owner == iota((256, 512), 1) + k * 512
        coupled[...] += nn(
            hit.astype(F32).astype(BF), amp[pl.ds(pl.multiple_of(k * 512, 512), 512), :]
        )
        return carry

    lax.fori_loop(0, 5, pick, 0)

    first15 = pl.ds(0, 15)

    def row_exchange(slot, src, dst, rest):
        return Exchange(sems, slot, 16, r, row_at, src, dst, rest)

    def col_exchange(slot, src, dst, rest):
        return Exchange(sems, slot, 16, xz, col_at, src, dst, rest)

    def block_exchange(make, slot, src, dst):
        return make(slot, lambda t: src.at[t], lambda s: dst.at[s], dst.at[first15])

    amp0_row = block_exchange(row_exchange, 0, own0, in0)
    amp1_col = block_exchange(col_exchange, 1, own1, in1)
    amp0_col = block_exchange(col_exchange, 2, mid0, fin0)
    amp1_row = block_exchange(row_exchange, 3, mid1, fin1)
    lad0_col = block_exchange(col_exchange, 4, lad0, got0)
    lad1_row = block_exchange(row_exchange, 5, lad1, got1)
    lad0_row = block_exchange(row_exchange, 6, turn0, back0)
    lad1_col = block_exchange(col_exchange, 7, turn1, back1)
    core_row = row_exchange(
        8,
        lambda t: core_parts.at[x, zh, r],
        lambda s: core_parts.at[x, zh, s],
        core_parts.at[x, zh, first15],
    )
    fac_row = row_exchange(
        9,
        lambda t: points.at[core, r, x],
        lambda s: points.at[core, s, x],
        points.at[core, first15, x],
    )
    hh_row = row_exchange(
        10,
        lambda t: rows.at[core, x, r],
        lambda s: rows.at[core, x, s],
        rows.at[core, x, first15],
    )

    def fac_part(slot, d):
        t = lax.rem(x + d, 4)
        return Swap(sems, slot, core, points.at[core, :, t], lambda s: points.at[s, :, t])

    def hh_part(slot, d):
        t = lax.rem(x + d, 4)
        return Swap(sems, slot, core, rows.at[core, t], lambda s: rows.at[s, t])

    fac_swaps = [fac_part(slot, d) for d, slot in enumerate((11, 51, 52, 53))]
    hh_swaps = [hh_part(slot, d) for d, slot in enumerate((12, 55, 56, 57))]
    amp_swap = Swap(sems, 13, core, whole.at[core], lambda s: whole.at[s])
    lad_swaps = [
        Swap(sems, slot, core, give.at[h], lambda s, h=h: take.at[h])
        for h, slot in enumerate((14, 54))
    ]
    fac_x = RingOfFour(
        sems,
        15,
        x,
        lambda t: points.at[core, :, t],
        lambda t, h: points.at[core, pl.ds(h * 8, 8), t],
    )
    hh_x = RingOfFour(
        sems, 19, x, lambda t: rows.at[core, t], lambda t, h: rows.at[core, t, pl.ds(h * 8, 8)]
    )

    def core_ring(d):
        z = lax.rem(zh + 4 - d, 4)
        return RingOfFour(
            sems,
            23 + 4 * d,
            x,
            lambda t: core_parts.at[t, z],
            lambda t, h: core_parts.at[t, z, pl.ds(h * 8, 8)],
        )

    core_rings = [core_ring(d) for d in range(4)]

    def core_step(d):
        def copy(place):
            part = core_parts.at[x, place]
            return remote(part, part, sems, 39 + d, {"zh": lax.rem(zh + d, 4)})

        return Single(lambda: copy(zh), lambda: copy(lax.rem(zh + 4 - d, 4)))

    core_zh = {d: core_step(d) for d in (1, 3, 2)}

    def piece_step(d, c):
        def copy(to_zh, to_core, slot_zh, slot_core):
            return remote(
                chunk.at[to_core],
                pieces.at[slot_zh, slot_core],
                sems,
                43 + d * 2 + c,
                {"zh": to_zh, "core": to_core},
            )

        peer = core if c == 0 else other
        source = lax.rem(zh + 4 - d, 4)
        return Single(
            lambda: copy(lax.rem(zh + d, 4), peer, zh, core),
            lambda: copy(source, peer, source, peer),
        )

    hops = [piece_step(d, c) for d in range(4) for c in range(2) if d or c]

    pl.semaphore_wait(barrier, 34)
    for hop in hops:
        hop.start()
    core_row.start()
    lax.fori_loop(5, 8, pick, 0)
    own[...] = coupled[...].astype(BF)
    own0[...] = own[:, :256].reshape(16, 16, 256)
    own1[...] = nn(swap, own[:, 256:]).astype(BF).reshape(16, 16, 256)
    amp0_row.start()
    amp1_col.start()
    in0[r] = own0[r]
    in1[xz] = own1[xz]
    fetches[3].wait()
    rows[core, x, r] = hh[:, pl.ds(pl.multiple_of((core * 4 + x) * 512, 512), 512)]
    order[...] = order_matrix()

    for hop in hops:
        hop.wait_recv()
    point = iota((16, 256), 0)
    tile16 = jnp.zeros((16, 256), F32)
    for a in range(4):
        for b in range(2):
            for j in range(2):
                tile16 = jnp.where(
                    point == a * 4 + b * 2 + j, pieces[a, b, pl.ds(j, 1), :], tile16
                )
    points[core, r, x] = tile16.astype(BF)
    fac_row.start()

    core_row.wait_recv()
    for step in core_zh.values():
        step.start()
    core_rings[0].start()

    amp0_row.wait_recv()
    mid0[...] = nn(swap, in0[...].reshape(256, 256)).astype(BF).reshape(16, 16, 256)
    amp0_col.start()
    fin0[xz] = mid0[xz]
    amp1_col.wait_recv()
    mid1[...] = nn(swap, in1[...].reshape(256, 256)).astype(BF).reshape(16, 16, 256)
    amp1_row.start()
    fin1[r] = mid1[r]

    fac_row.wait_recv()
    fac_x.start()
    fac_swaps[0].start()
    core_zh[1].wait_recv()
    core_rings[1].start()
    fac_x.forward()
    fac_swaps[1].start()
    fac_swaps[3].start()
    hh_row.start()
    core_zh[3].wait_recv()
    core_rings[3].start()
    core_zh[2].wait_recv()
    core_rings[2].start()

    amp0_col.wait_recv()
    whole[core, :, :256] = fin0[...].reshape(256, 256)
    amp1_row.wait_recv()
    whole[core, :, 256:] = nn(swap, fin1[...].reshape(256, 256)).astype(BF)
    amp_swap.start()

    def my_points(h):
        return points[h, :, pl.ds(core * 2, 2)].reshape(512, 256)

    def lanes_half(h):
        return pl.ds(pl.multiple_of(h * 256, 256), 256)

    def half_from(h, t):
        left = whole[:, :, lanes_half(h)].reshape(512, 256)
        return nt(left, points[h, pl.ds(t * 4, 4)].reshape(256, 256))

    core_rings[0].forward()
    core_rings[1].forward()
    fac_x.wait_recv()
    fac_swaps[2].start()
    core_rings[3].forward()
    amp_swap.wait_recv()

    for t in range(4):
        half_part[:, t * 256 : t * 256 + 256] = half_from(core, t)
    part0[...] = nt(my_points(core), order[:, lanes_half(core)])
    part1[...] = nt(order[:, lanes_half(core)], my_points(core))

    core_rings[2].forward()
    hh_row.wait_recv()
    hh_x.start()
    hh_swaps[0].start()
    for part in fac_swaps:
        part.wait_recv()

    for t in range(4):
        cols = slice(t * 256, t * 256 + 256)
        half[:, cols] = (half_part[:, cols] + half_from(other, t)).astype(BF)
    order0[...] = (part0[...] + nt(my_points(other), order[:, lanes_half(other)])).astype(BF)
    order1[...] = (part1[...] + nt(order[:, lanes_half(other)], my_points(other))).astype(BF)
    for t in range(4):
        cols = slice(t * 256, t * 256 + 256)
        middle[:, :, :, cols] = nn(order0[...], half[:, cols]).reshape(16, 2, 16, 256)

    low = iota((64, 128), 1) < 64

    def weigh(block):
        at = pl.ds(block * 4, 4)
        for t in range(8):
            cols = slice(t * 128, t * 128 + 128)
            even = core_parts[block, :, 2 * t].reshape(64, 128).astype(F32)
            odd = core_parts[block, :, 2 * t + 1].reshape(64, 128).astype(F32)
            top = jnp.where(low, even, pltpu.roll(odd, 64, 1)).reshape(4, 16, 128)
            bottom = jnp.where(low, pltpu.roll(even, 64, 1), odd).reshape(4, 16, 128)
            weighted[at, 0, :, cols] = (top * middle[at, 0, :, cols]).astype(BF)
            weighted[at, 1, :, cols] = (bottom * middle[at, 1, :, cols]).astype(BF)

    def weigh_near(i, carry):
        weigh(lax.rem(x + i + i // 2, 4))
        return carry

    lax.fori_loop(0, 3, weigh_near, 0)
    for ring in core_rings:
        ring.wait_recv()
    weigh(lax.rem(x + 2, 4))

    def back_of(side):
        at = pl.ds(pl.multiple_of(side * 256, 256), 256)
        return nn(order1[at, :], weighted[...].reshape(512, 1024)).astype(BF)

    def ladder_of(back, h):
        return nn(back, points[h].reshape(1024, 256))

    back = back_of(other)
    for h in range(2):
        give[h] = ladder_of(back, h).astype(BF)
        lad_swaps[h].start()
    back = back_of(core)
    mine = ladder_of(back, 0)
    lad_swaps[0].wait_recv()
    lad0[...] = (mine + take[0].astype(F32)).astype(BF).reshape(16, 16, 256)
    lad0_col.start()
    mine = ladder_of(back, 1)
    lad_swaps[1].wait_recv()
    mine = (mine + take[1].astype(F32)).astype(BF)
    lad1[...] = nn(swap, mine).astype(BF).reshape(16, 16, 256)
    lad1_row.start()
    hh_x.forward()
    hh_swaps[1].start()
    hh_swaps[3].start()
    got0[xz] = lad0[xz]
    got1[r] = lad1[r]

    lad0_col.wait_recv()
    turn0[...] = nn(swap, got0[...].reshape(256, 256)).astype(BF).reshape(16, 16, 256)
    lad0_row.start()
    back0[r] = turn0[r]
    lad1_row.wait_recv()
    turn1[...] = nn(swap, got1[...].reshape(256, 256)).astype(BF).reshape(16, 16, 256)
    lad1_col.start()
    back1[xz] = turn1[xz]

    hh_x.wait_recv()
    hh_swaps[2].start()
    for part in hh_swaps:
        part.wait_recv()
    coupled[...] = jnp.zeros((256, 512), F32)

    def couple(k, carry):
        coupled[...] += nn(
            rows[k // 4, k % 4].reshape(256, 512),
            amp[pl.ds(pl.multiple_of(k * 512, 512), 512), :],
        )
        return carry

    lax.fori_loop(0, 8, couple, 0)
    for fetch in fetches[4:]:
        fetch.wait()
    device = r * 32 + xz * 2 + core
    vir_mine = jnp.sum(
        jnp.where(iota((1, 512), 1) == device, vir[...], 0.0), axis=1, keepdims=True
    )
    orbital = iota((256, 64), 1)
    first_hit = (owner // 64) == orbital
    second_hit = (owner % 64) == orbital
    occ_first = jnp.sum(jnp.where(first_hit, occ[...], 0.0), axis=1, keepdims=True)
    occ_second = jnp.sum(jnp.where(second_hit, occ[...], 0.0), axis=1, keepdims=True)
    occ_pair = occ_first + occ_second
    coupled[...] += integrals[...].astype(F32)

    def finish(k, lad):
        cols = slice(k * 256, k * 256 + 256)
        denom = (vir_mine + vir[:, cols]) - occ_pair
        rest = coupled[:, cols] + lad.astype(F32)
        update = 0.4 * own[:, cols].astype(F32) + 0.6 * rest / denom
        out[:, cols] = update.astype(BF)

    lad0_row.wait_recv()
    finish(0, back0[...].reshape(256, 256))
    lad1_col.wait_recv()
    finish(1, nn(swap, back1[...].reshape(256, 256)))

    for move in (
        *hops, *core_zh.values(), core_row, *core_rings, fac_row, fac_x, *fac_swaps, hh_row, hh_x, *hh_swaps,
        amp0_row, amp1_col, amp0_col, amp1_row, amp_swap, *lad_swaps,
        lad0_col, lad1_row, lad0_row, lad1_col,
    ):
        move.wait_send()


def per_device(
    amplitudes, integrals, hh_coupling, thc_factor, thc_core, occ_energy, vir_energy, pair_owner
):
    cube = pltpu.VMEM((16, 16, 256), BF)
    scratch = [
        pltpu.VMEM((4096, 512), BF),
        pltpu.VMEM((256, 512), BF),
        pltpu.VMEM((16, 4096), BF),
        pltpu.VMEM((2, 512), BF),
        pltpu.VMEM((32, 64), F32),
        pltpu.VMEM((1, 64), F32),
        pltpu.VMEM((1, 512), F32),
        pltpu.VMEM((1, 256), jnp.int32),
        pltpu.VMEM((256, 512), BF),
        *[cube] * 8,
        pltpu.VMEM((2, 256, 512), BF),
        pltpu.VMEM((2, 2, 256), F32),
        pltpu.VMEM((4, 2, 2, 256), F32),
        pltpu.VMEM((2, 16, 4, 16, 256), BF),
        pltpu.VMEM((4, 4, 16, 16, 128), BF),
        pltpu.VMEM((2, 4, 16, 16, 512), BF),
        pltpu.VMEM((512, 1024), BF),
        pltpu.VMEM((512, 512), BF),
        pltpu.VMEM((512, 512), BF),
        pltpu.VMEM((512, 512), BF),
        pltpu.VMEM((512, 1024), F32),
        pltpu.VMEM((512, 512), F32),
        pltpu.VMEM((512, 512), F32),
        pltpu.VMEM((16, 2, 16, 1024), F32),
        pltpu.VMEM((16, 2, 16, 1024), BF),
        pltpu.VMEM((2, 256, 256), BF),
        pltpu.VMEM((2, 256, 256), BF),
        *[cube] * 8,
        pltpu.VMEM((256, 512), F32),
        pltpu.SemaphoreType.DMA((15,)),
        pltpu.SemaphoreType.DMA((N_MOVES,)),
        pltpu.SemaphoreType.DMA((N_MOVES,)),
    ]
    return pl.pallas_call(
        kernel,
        out_shape=jax.ShapeDtypeStruct((256, 512), BF),
        in_specs=[pl.BlockSpec(memory_space=pltpu.HBM)] * 8,
        out_specs=pl.BlockSpec(memory_space=pltpu.VMEM),
        scratch_shapes=scratch,
        compiler_params=pltpu.CompilerParams(
            collective_id=0, has_side_effects=True, vmem_limit_bytes=50000000
        ),
    )(
        *(
            pltpu.with_memory_space_constraint(operand, pltpu.HBM)
            for operand in (
                amplitudes,
                integrals,
                hh_coupling,
                thc_factor.T,
                thc_core,
                occ_energy.reshape(1, -1),
                vir_energy.reshape(1, -1),
                pair_owner.reshape(1, -1),
            )
        )
    )


def solution(mesh):
    finer = Mesh(mesh.devices.reshape(2, 8, 4, 4, 2), AXES)
    wide = P(None, ROW + COL)
    in_specs = (wide, wide, P(ROW, None), wide, P(COL, ROW), P(), P(), P())
    return jax.shard_map(
        per_device, mesh=finer, in_specs=in_specs, out_specs=wide, check_vma=False
    )
```
